32 devices in a mesh: seq: 2 (over x), mp: 4 (over y, core), dp: 4 (over z).
Axes of the slice: x: 2, y: 2, z: 4, core: 2. Of those that a mesh axis runs over, the one named last changes fastest.
Arguments:
- tokens: bfloat16 [16384, 2048], P(('dp', 'seq'), 'mp'), parts along dimension 0, may hold values from -6 to 6
- w_query: bfloat16 [2048, 2048], P(None, 'mp'), may hold values from -0.125 to 0.125
- w_key: bfloat16 [2048, 2048], P(None, 'mp'), may hold values from -0.125 to 0.125
- w_value: bfloat16 [2048, 2048], P(None, 'mp'), may hold values from -0.125 to 0.125
- w_gate: bfloat16 [2048, 2048], P(None, 'mp'), may hold values from -0.125 to 0.125
- decay_exponent: int32 [16], P('mp'), may hold values from 5 to 16
- forget: float32 [16384, 16], P(('dp', 'seq'), 'mp'), parts along dimension 0, may hold values from 0 to 0.69
- norm_gain: float32 [2048], replicated, may hold values from 0.1 to 1.9
Outputs:
- retained: bfloat16 [16384, 2048], P(('dp', 'seq', 'mp')), parts along dimension 0
The draws below stay inside these ranges and needn't reach their ends.
There are 4 independent parts, one for each index of `dp`. The reference program is written for one: setup_inputs(seed, part) draws one part's arguments, and reference() takes and returns one part's arrays. A program takes and returns all parts, laid end to end along the dimension named above; an argument that names none is the same for every part. Nothing has to cross between parts.
All inputs are finite; a program needn't handle non-finite values.
Results may differ from the reference program's by a relative error of at most 0.015.
Values may be sent and summed in bfloat16 or wider, within the bound.
A program may use at most 64 MiB of HBM per device.

```python
import jax
import jax.numpy as jnp
from jax import lax

D = 2048
HEADS = 16
DH = 128
TOKENS = 4096
FEATURES = 2048


def draw_forget(key, part):
    first_key, second_key = jax.random.split(jax.random.fold_in(key, 11))
    chance = jax.random.uniform(first_key, (TOKENS, HEADS), jnp.float32)
    amount = jax.random.uniform(second_key, (TOKENS, HEADS), jnp.float32, 0.22, 0.69)
    return jnp.where(chance < 6.0 / TOKENS, amount, 0.0).astype(jnp.float32)


def with_ends(entries, key, low, high):
    spot = [jax.random.randint(jax.random.fold_in(key, axis), (), 0, length) for axis, length in enumerate(entries.shape)]
    longest = entries.shape.index(max(entries.shape))
    next_to = spot[:longest] + [(spot[longest] + 1) % entries.shape[longest]] + spot[longest + 1:]
    return entries.at[tuple(spot)].set(low).at[tuple(next_to)].set(high)


def level_of(rng, extent, shards, smallest, top_value):
    level, own = 1.0, jax.random.fold_in(rng, 6)
    for axis_at, shards_of in shards:
        heights = jnp.exp(jax.random.uniform(jax.random.fold_in(own, axis_at), (shards_of,), jnp.float32, smallest / len(shards), top_value / len(shards)))
        level = level * jnp.repeat(heights, extent[axis_at] // shards_of).reshape([-1 if axis == axis_at else 1 for axis in range(len(extent))])
    return level


def normal_values(key, extent, spread, reach, shards=(), kind=jnp.bfloat16):
    level = level_of(key, extent, shards, -0.22, 0.18) if shards else 1.0
    values = jax.random.normal(key, extent, jnp.float32) * spread * level
    return jnp.minimum(jnp.maximum(values, -reach), reach).astype(kind)


def setup_inputs(seed: int = 0, part: int = 0) -> dict:
    keys = jax.random.split(jax.random.key(seed), 9)
    part_splits = jax.random.split(jax.random.fold_in(keys[8], part), 9)
    return {
        "tokens": normal_values(part_splits[0], (TOKENS, D), 1.0, 6.0, ((0, 2), (1, 4))),
        "w_query": normal_values(keys[1], (D, FEATURES), D ** -0.5, 0.125, ((1, 4),)),
        "w_key": normal_values(keys[2], (D, FEATURES), D ** -0.5, 0.125, ((1, 4),)),
        "w_value": normal_values(keys[3], (D, FEATURES), D ** -0.5, 0.125, ((1, 4),)),
        "w_gate": normal_values(keys[4], (D, FEATURES), D ** -0.5, 0.125, ((1, 4),)),
        "decay_exponent": with_ends(jax.random.randint(keys[5], (HEADS,), 5, 17), jax.random.fold_in(keys[5], 1), 5, 16).astype(jnp.int32),
        "forget": draw_forget(jax.random.fold_in(jax.random.fold_in(keys[8], part), 71), part),
        "norm_gain": jnp.clip(1.0 + 0.18 * jax.random.normal(keys[7], (FEATURES,), jnp.float32), 0.1, 1.9),
    }


def retention(queries, key_rows, values, logdecay):
    seq_rows = queries.shape[0]
    head_count = logdecay.shape[1]
    head_width = queries.shape[1] // head_count
    block_rows = 512 if seq_rows % 512 == 0 else seq_rows
    block_count = seq_rows // block_rows

    def shaped(source):
        return source.reshape(block_count, block_rows, head_count, head_width)
    decays = logdecay.reshape(block_count, block_rows, head_count)
    position = lax.broadcasted_iota(jnp.int32, (block_rows, block_rows), 0)
    earlier = lax.broadcasted_iota(jnp.int32, (block_rows, block_rows), 1)
    causal = position >= earlier

    def advance(kv_state, pieces):
        query_blk, key_blk, value_blk, decay_blk = pieces
        running = jnp.cumsum(decay_blk, axis=0)
        heads_first = running.T
        log_gap = heads_first[:, :, None] - heads_first[:, None, :]
        decay_mask = jnp.where(causal[None], jnp.exp(jnp.where(causal[None], log_gap, 0.0)), 0.0)
        query_float = query_blk.astype(jnp.float32)
        key_float = key_blk.astype(jnp.float32)
        value_float = value_blk.astype(jnp.float32)
        scores = (jnp.einsum('tha,sha->hts', query_float, key_float) * decay_mask).astype(jnp.bfloat16)
        inner = jnp.einsum('hts,shb->thb', scores.astype(jnp.float32), value_float)
        carried = jnp.einsum('tha,hab->thb', query_float * jnp.exp(running)[:, :, None], kv_state, precision=lax.Precision.HIGHEST)
        key_scaled = key_float * jnp.exp(running[-1:] - running)[:, :, None]
        kv_state = jnp.exp(running[-1])[:, None, None] * kv_state + jnp.einsum('sha,shb->hab', key_scaled, value_float, precision=lax.Precision.HIGHEST)
        return (kv_state, (inner + carried).astype(jnp.bfloat16))
    initial = jnp.zeros((head_count, head_width, head_width), jnp.float32)
    final_state, outputs = lax.scan(advance, initial, (shaped(queries), shaped(key_rows), shaped(values), decays))
    return outputs.reshape(seq_rows, head_count * head_width)

def reference(tokens, w_query, w_key, w_value, w_gate, decay_exponent, forget, norm_gain):
    queries = jnp.dot(tokens, w_query, preferred_element_type=jnp.float32).astype(jnp.bfloat16)
    key_rows = (jnp.dot(tokens, w_key, preferred_element_type=jnp.float32) * DH ** (-0.5)).astype(jnp.bfloat16)
    values = jnp.dot(tokens, w_value, preferred_element_type=jnp.float32).astype(jnp.bfloat16)
    gate = jnp.dot(tokens, w_gate, preferred_element_type=jnp.float32).astype(jnp.bfloat16)
    rate = jnp.log1p(-jnp.exp2(-decay_exponent.astype(jnp.float32)))
    logdecay = rate[None, :] - forget
    output = retention(queries, key_rows, values, logdecay).astype(jnp.float32)
    squares = lax.optimization_barrier(jnp.mean(output * output, axis=1))
    rstd = lax.rsqrt(squares + 1e-06)
    gated = jax.nn.silu(gate.astype(jnp.float32)) * output * rstd[:, None] * norm_gain[None, :]
    return gated.astype(jnp.bfloat16)
```

```python
import functools

import jax
import jax.numpy as jnp
from jax import lax
from jax.experimental import pallas as pl
from jax.experimental.pallas import tpu as pltpu
from jax.sharding import PartitionSpec as P

DH = 128
MESH = pl.DeviceIdType.MESH
F32 = jnp.float32
BF16 = jnp.bfloat16


def contract(a, b, dims):
    return lax.dot_general(a, b, ((dims[0], dims[1]), ((), ())), preferred_element_type=F32)


def kernel(
    n_mp, n_seq, heads, rows,
    tokens, wq, wk, wv, wg, decay, gain, out,
    x, w, local_out, q_in, moved, got, sq_out, sq_got, gates, state, enter, state_out, state_got, offset,
    weight_sem, own_sem, y_send, y_recv, d_send, d_recv, s_send, s_recv, m_send, m_recv, q_send, q_recv,
):
    me = lax.axis_index("mp")
    place = lax.axis_index("seq")
    chips = n_mp // 2
    chip, core = me // 2, me % 2
    partner = chip * 2 + (1 - core)
    seq_rows, width = tokens.shape
    chunks = seq_rows // rows
    own_rows = seq_rows // n_mp
    parts = own_rows // rows
    head_width = width // heads

    weights = [pltpu.make_async_copy(src, w.at[i], weight_sem.at[i]) for i, src in enumerate((wq, wk, wv, wg))]

    def columns(block):
        return pl.ds(pl.multiple_of(block * width, width), width)

    def at_rows(c):
        return pl.ds(pl.multiple_of(c * rows, rows), rows)

    def own_copy(c):
        return pltpu.make_async_copy(tokens.at[at_rows(c), :], x.at[at_rows(c), columns(me)], own_sem.at[c])

    def far(step):
        return lax.rem(chip + step, chips) * 2 + core

    def back(step):
        return lax.rem(chip + chips - step, chips) * 2 + core

    def y_copy(c, step):
        return pltpu.make_async_remote_copy(
            src_ref=tokens.at[at_rows(c), :], dst_ref=x.at[at_rows(c), columns(me)],
            send_sem=y_send.at[c, step], recv_sem=y_recv.at[c, step],
            device_id={"mp": far(step)}, device_id_type=MESH)

    def y_arrival(c, step):
        return pltpu.make_async_remote_copy(
            src_ref=tokens.at[at_rows(c), :], dst_ref=x.at[at_rows(c), columns(back(step))],
            send_sem=y_send.at[c, step], recv_sem=y_recv.at[c, step],
            device_id={"mp": far(step)}, device_id_type=MESH)

    def d_copy(c, step):
        block = me if step == 0 else back(step)
        source = tokens.at[at_rows(c), :] if step == 0 else x.at[at_rows(c), columns(block)]
        return pltpu.make_async_remote_copy(
            src_ref=source, dst_ref=x.at[at_rows(c), columns(block)],
            send_sem=d_send.at[c, step], recv_sem=d_recv.at[c, step],
            device_id={"mp": partner}, device_id_type=MESH)

    def d_arrival(c, step):
        block = partner if step == 0 else lax.rem(chip + chips - step, chips) * 2 + (1 - core)
        there = x.at[at_rows(c), columns(block)]
        return pltpu.make_async_remote_copy(
            src_ref=there, dst_ref=there, send_sem=d_send.at[c, step], recv_sem=d_recv.at[c, step],
            device_id={"mp": partner}, device_id_type=MESH)

    barrier = pltpu.get_barrier_semaphore()
    for other in range(1, n_mp):
        pl.semaphore_signal(barrier, inc=1, device_id={"mp": lax.rem(me + other, n_mp)}, device_id_type=MESH)

    @pl.when(place > 0)
    def _():
        pl.semaphore_signal(barrier, inc=1, device_id={"seq": place - 1}, device_id_type=MESH)

    @pl.when(place < n_seq - 1)
    def _():
        pl.semaphore_signal(barrier, inc=1, device_id={"seq": place + 1}, device_id_type=MESH)

    for i in range(3):
        weights[i].start()
    pl.loop(0, chunks)(lambda c: own_copy(c).start())
    weights[3].start()

    neighbours = jnp.minimum(place, 1) + jnp.minimum(n_seq - 1 - place, 1)
    pl.semaphore_wait(barrier, n_mp - 1 + neighbours)

    @pl.loop(0, chunks)
    def _(c):
        for step in range(1, chips):
            y_copy(c, step).start()
        d_copy(c, 0).start()

    state[...] = jnp.zeros_like(state)
    offset[...] = jnp.zeros_like(offset)
    for i in range(3):
        weights[i].wait()

    later = lax.broadcasted_iota(jnp.int32, (rows, rows), 0)
    earlier = lax.broadcasted_iota(jnp.int32, (rows, rows), 1)
    causal = later >= earlier
    summing = (later <= earlier).astype(F32)

    @pl.loop(0, chunks)
    def _(c):
        here = at_rows(c)
        for step in range(1, chips):
            y_arrival(c, step).wait_recv()
            d_copy(c, step).start()
        own_copy(c).wait()
        running = jnp.dot(decay[:, here], summing, precision=lax.Precision.HIGHEST, preferred_element_type=F32)
        by_row = running.T
        last = running[:, rows - 1 :]
        before = offset[...]
        for step in range(chips):
            d_arrival(c, step).wait_recv()
        piece = x[here, :]
        query = jnp.dot(piece, w[0], preferred_element_type=F32).astype(BF16)
        key = (jnp.dot(piece, w[1], preferred_element_type=F32) * DH ** (-0.5)).astype(BF16)
        value = jnp.dot(piece, w[2], preferred_element_type=F32).astype(BF16)
        for h in range(heads):
            part = slice(h * head_width, (h + 1) * head_width)
            q, k, v = query[:, part], key[:, part], value[:, part]
            col = by_row[:, h : h + 1]
            mask = jnp.exp(jnp.where(causal, col - running[h : h + 1, :], -1e30))
            scores = (contract(q, k, ((1,), (1,))) * mask).astype(BF16)
            grown = state[h]
            qf = q.astype(F32)
            carried = jnp.dot((qf * jnp.exp(col)).astype(BF16), grown.astype(BF16), preferred_element_type=F32)
            local_out[here, part] = jnp.dot(scores, v, preferred_element_type=F32) + carried
            q_in[here, part] = (qf * jnp.exp(col + before[h : h + 1, 0:1])).astype(BF16)
            faded = (k.astype(F32) * jnp.exp(last[h : h + 1, :] - col)).astype(BF16)
            state[h] = jnp.exp(last[h : h + 1, :]) * grown + contract(faded, v, ((0,), (0,)))
        offset[...] = before + last

    s_copy = pltpu.make_async_remote_copy(
        src_ref=state_out, dst_ref=state_got, send_sem=s_send, recv_sem=s_recv,
        device_id={"seq": lax.rem(place + 1, n_seq)}, device_id_type=MESH)

    @pl.when(place == 0)
    def _():
        enter[...] = jnp.zeros_like(enter)
        state_out[...] = state[...].astype(BF16)
        if n_seq > 1:
            s_copy.start()

    def owner(o):
        t, s = o // 2, o % 2
        return lax.rem(chip + t + 1, chips) * 2 + lax.rem(core + s + (t + 1) // chips, 2)

    def gate_of(step):
        o, r = lax.rem(step, n_mp), step // n_mp
        here = at_rows(owner(o) * parts + r)
        g = jnp.dot(x[here, :], w[3], preferred_element_type=F32).astype(BF16).astype(F32)
        gates[...] = g / (1.0 + jnp.exp(-g))

    weights[3].wait()
    gate_of(0)

    @pl.when(place > 0)
    def _():
        s_copy.wait_recv()
        enter[...] = state_got[...]

    if n_seq > 2:
        @pl.when(jnp.logical_and(place > 0, place < n_seq - 1))
        def _():
            for h in range(heads):
                total = jnp.exp(offset[h : h + 1, 0:1])
                state_out[h] = (total * enter[h].astype(F32) + state[h]).astype(BF16)
            s_copy.start()

    def m_copy(o, r):
        to = owner(o)
        return pltpu.make_async_remote_copy(
            src_ref=moved.at[at_rows(to * parts + r), :], dst_ref=got.at[me, at_rows(r), :],
            send_sem=m_send.at[o, r], recv_sem=m_recv.at[me, r],
            device_id={"mp": to}, device_id_type=MESH)

    def q_copy(o, r):
        to = owner(o)
        return pltpu.make_async_remote_copy(
            src_ref=sq_out.at[to * parts + r], dst_ref=sq_got.at[me, r],
            send_sem=q_send.at[o, r], recv_sem=q_recv.at[me, r],
            device_id={"mp": to}, device_id_type=MESH)

    steps = n_mp * parts
    ones = jnp.ones((8, width), BF16)

    @pl.loop(0, steps)
    def _(step):
        o, r = lax.rem(step, n_mp), step // n_mp
        block = owner(o) * parts + r
        here = at_rows(block)
        squares = jnp.zeros((8, rows), F32)
        for h in range(heads):
            part = slice(h * head_width, (h + 1) * head_width)
            whole = local_out[here, part] + jnp.dot(q_in[here, part], enter[h], preferred_element_type=F32)
            whole = whole.astype(BF16).astype(F32)
            square = whole * whole
            high = square.astype(BF16)
            low = (square - high.astype(F32)).astype(BF16)
            unit = ones[:, part]
            squares += contract(unit, high, ((1,), (1,))) + contract(unit, low, ((1,), (1,)))
            moved[here, part] = (gates[:, part] * whole).astype(BF16)
        sq_out[block] = squares

        @pl.when(o < n_mp - 1)
        def _():
            q_copy(o, r).start()
            m_copy(o, r).start()

        @pl.when(o == n_mp - 1)
        def _():
            got[me, at_rows(r), :] = moved[here, :]
            sq_got[me, r] = squares

        @pl.when(step < steps - 1)
        def _():
            gate_of(step + 1)

    def m_arrival(source, r):
        there = got.at[source, at_rows(r), :]
        return pltpu.make_async_remote_copy(
            src_ref=there, dst_ref=there, send_sem=m_send.at[0, r], recv_sem=m_recv.at[source, r],
            device_id={"mp": partner}, device_id_type=MESH)

    def q_arrival(source, r):
        there = sq_got.at[source, r]
        return pltpu.make_async_remote_copy(
            src_ref=there, dst_ref=there, send_sem=q_send.at[0, r], recv_sem=q_recv.at[source, r],
            device_id={"mp": partner}, device_id_type=MESH)

    for r in range(parts):
        for other in range(1, n_mp):
            source = lax.rem(me + other, n_mp)
            q_arrival(source, r).wait_recv()
            m_arrival(source, r).wait_recv()
        total = sq_got[0, r]
        for source in range(1, n_mp):
            total += sq_got[source, r]
        scale = lax.rsqrt(total * (1.0 / (n_mp * width)) + 1e-06).T[:, 0:1]
        span = slice(r * rows, (r + 1) * rows)
        for source in range(n_mp):
            part = slice(source * width, (source + 1) * width)
            out[span, part] = (got[source, span, :].astype(F32) * scale * gain[:, part]).astype(BF16)

    @pl.loop(0, chunks)
    def _(c):
        for step in range(1, chips):
            y_copy(c, step).wait_send()
        for step in range(chips):
            d_copy(c, step).wait_send()

    @pl.loop(0, n_mp - 1)
    def _(o):
        for r in range(parts):
            q_copy(o, r).wait_send()
            m_copy(o, r).wait_send()

    if n_seq > 1:
        @pl.when(place < n_seq - 1)
        def _():
            s_copy.wait_send()


def body(n_mp, n_seq, tokens, w_query, w_key, w_value, w_gate, decay_exponent, forget, norm_gain):
    seq_rows, width = tokens.shape
    features = w_query.shape[0]
    heads = decay_exponent.shape[0]
    own_rows = seq_rows // n_mp
    rows = 256 if own_rows % 256 == 0 else own_rows
    chunks, parts = seq_rows // rows, own_rows // rows
    rate = jnp.log1p(-jnp.exp2(-decay_exponent.astype(F32)))
    lanes = -(-heads // 8) * 8
    decay = jnp.pad((rate[None, :] - forget).T, ((0, lanes - heads), (0, 0)))
    hbm, vmem = pl.BlockSpec(memory_space=pl.ANY), pl.BlockSpec(memory_space=pltpu.VMEM)
    dma = pltpu.SemaphoreType.DMA
    chips = n_mp // 2
    return pl.pallas_call(
        functools.partial(kernel, n_mp, n_seq, heads, rows),
        out_shape=jax.ShapeDtypeStruct((own_rows, features), BF16),
        in_specs=[hbm] * 5 + [vmem] * 2,
        out_specs=vmem,
        scratch_shapes=[
            pltpu.VMEM((seq_rows, features), BF16),
            pltpu.VMEM((4, features, width), BF16),
            pltpu.VMEM((seq_rows, width), F32),
            pltpu.VMEM((seq_rows, width), BF16),
            pltpu.VMEM((seq_rows, width), BF16),
            pltpu.VMEM((n_mp, own_rows, width), BF16),
            pltpu.VMEM((chunks, 8, rows), F32),
            pltpu.VMEM((n_mp, parts, 8, rows), F32),
            pltpu.VMEM((rows, width), F32),
            pltpu.VMEM((heads, DH, DH), F32),
            pltpu.VMEM((heads, DH, DH), BF16),
            pltpu.VMEM((heads, DH, DH), BF16),
            pltpu.VMEM((heads, DH, DH), BF16),
            pltpu.VMEM((lanes, 128), F32),
            dma((4,)),
            dma((chunks,)),
            dma((chunks, chips)),
            dma((chunks, chips)),
            dma((chunks, chips)),
            dma((chunks, chips)),
            dma,
            dma,
            dma((n_mp, parts)),
            dma((n_mp, parts)),
            dma((n_mp, parts)),
            dma((n_mp, parts)),
        ],
        compiler_params=pltpu.CompilerParams(
            collective_id=0, has_side_effects=True, vmem_limit_bytes=60 * 1024 * 1024
        ),
    )(tokens, w_query, w_key, w_value, w_gate, decay, norm_gain[None, :])


def solution(mesh):
    placed = (
        P(("dp", "seq"), "mp"),
        P(None, "mp"),
        P(None, "mp"),
        P(None, "mp"),
        P(None, "mp"),
        P("mp"),
        P(("dp", "seq"), "mp"),
        P(),
    )
    return jax.shard_map(
        functools.partial(body, mesh.shape["mp"], mesh.shape["seq"]),
        mesh=mesh,
        in_specs=placed,
        out_specs=P(("dp", "seq", "mp"), None),
        check_vma=False,
    )
```

```python
import functools

import jax
import jax.numpy as jnp
from jax import lax
from jax.experimental import pallas as pl
from jax.experimental.pallas import tpu as pltpu
from jax.sharding import PartitionSpec as P

DH = 128
MESH = pl.DeviceIdType.MESH
F32 = jnp.float32
BF16 = jnp.bfloat16


def contract(a, b, dims):
    return lax.dot_general(a, b, ((dims[0], dims[1]), ((), ())), preferred_element_type=F32)


def kernel(
    n_mp, n_seq, heads, rows,
    tokens, wq, wk, wv, wg, forget, rate, gain, out,
    x, w, local_out, q_in, moved, got, sq_out, sq_got, gates, state, held, enter, state_out, state_got, offset,
    weight_sem, own_sem, y_send, y_recv, d_send, d_recv, s_send, s_recv, m_send, m_recv, q_send, q_recv,
):
    me = lax.axis_index("mp")
    place = lax.axis_index("seq")
    chips = n_mp // 2
    chip, core = me // 2, me % 2
    partner = chip * 2 + (1 - core)
    seq_rows, width = tokens.shape
    chunks = seq_rows // rows
    own_rows = seq_rows // n_mp
    parts = own_rows // rows
    head_width = width // heads

    weights = [pltpu.make_async_copy(src, w.at[i], weight_sem.at[i]) for i, src in enumerate((wq, wk, wv, wg))]

    def columns(block):
        return pl.ds(pl.multiple_of(block * width, width), width)

    def at_rows(c):
        return pl.ds(pl.multiple_of(c * rows, rows), rows)

    def own_copy(c):
        return pltpu.make_async_copy(tokens.at[at_rows(c), :], x.at[at_rows(c), columns(me)], own_sem.at[c])

    def far(step):
        return lax.rem(chip + step, chips) * 2 + core

    def back(step):
        return lax.rem(chip + chips - step, chips) * 2 + core

    def y_copy(c, step):
        return pltpu.make_async_remote_copy(
            src_ref=tokens.at[at_rows(c), :], dst_ref=x.at[at_rows(c), columns(me)],
            send_sem=y_send.at[c, step], recv_sem=y_recv.at[c, step],
            device_id={"mp": far(step)}, device_id_type=MESH)

    def y_arrival(c, step):
        return pltpu.make_async_remote_copy(
            src_ref=tokens.at[at_rows(c), :], dst_ref=x.at[at_rows(c), columns(back(step))],
            send_sem=y_send.at[c, step], recv_sem=y_recv.at[c, step],
            device_id={"mp": far(step)}, device_id_type=MESH)

    def d_copy(c, step):
        block = me if step == 0 else back(step)
        source = tokens.at[at_rows(c), :] if step == 0 else x.at[at_rows(c), columns(block)]
        return pltpu.make_async_remote_copy(
            src_ref=source, dst_ref=x.at[at_rows(c), columns(block)],
            send_sem=d_send.at[c, step], recv_sem=d_recv.at[c, step],
            device_id={"mp": partner}, device_id_type=MESH)

    def d_arrival(c, step):
        block = partner if step == 0 else lax.rem(chip + chips - step, chips) * 2 + (1 - core)
        there = x.at[at_rows(c), columns(block)]
        return pltpu.make_async_remote_copy(
            src_ref=there, dst_ref=there, send_sem=d_send.at[c, step], recv_sem=d_recv.at[c, step],
            device_id={"mp": partner}, device_id_type=MESH)

    barrier = pltpu.get_barrier_semaphore()
    for other in range(1, n_mp):
        pl.semaphore_signal(barrier, inc=1, device_id={"mp": lax.rem(me + other, n_mp)}, device_id_type=MESH)

    @pl.when(place > 0)
    def _():
        pl.semaphore_signal(barrier, inc=1, device_id={"seq": place - 1}, device_id_type=MESH)

    @pl.when(place < n_seq - 1)
    def _():
        pl.semaphore_signal(barrier, inc=1, device_id={"seq": place + 1}, device_id_type=MESH)

    for i in range(3):
        weights[i].start()
    pl.loop(0, chunks)(lambda c: own_copy(c).start())
    weights[3].start()

    neighbours = jnp.minimum(place, 1) + jnp.minimum(n_seq - 1 - place, 1)
    pl.semaphore_wait(barrier, n_mp - 1 + neighbours)

    @pl.loop(0, chunks)
    def _(c):
        for step in range(1, chips):
            y_copy(c, step).start()
        d_copy(c, 0).start()

    state[...] = jnp.zeros_like(state)
    offset[...] = jnp.zeros_like(offset)
    for i in range(3):
        weights[i].wait()

    later = lax.broadcasted_iota(jnp.int32, (rows, rows), 0)
    earlier = lax.broadcasted_iota(jnp.int32, (rows, rows), 1)
    causal = later >= earlier
    summing = (later <= earlier).astype(F32)
    exact = lax.Precision.HIGHEST

    s_copy = pltpu.make_async_remote_copy(
        src_ref=state_out, dst_ref=state_got, send_sem=s_send, recv_sem=s_recv,
        device_id={"seq": lax.rem(place + 1, n_seq)}, device_id_type=MESH)

    @pl.loop(0, chunks)
    def _(c):
        here = at_rows(c)
        for step in range(1, chips):
            y_arrival(c, step).wait_recv()
            d_copy(c, step).start()
        own_copy(c).wait()
        decay = rate[...] - forget[:, here]
        running = jnp.dot(decay, summing, precision=exact, preferred_element_type=F32)
        by_row = lax.dot_general(
            causal.astype(F32), decay, (((1,), (1,)), ((), ())), precision=exact, preferred_element_type=F32)
        last = running[:, rows - 1 :]
        before = offset[...]
        for step in range(chips):
            d_arrival(c, step).wait_recv()
        piece = x[here, :]
        key = (jnp.dot(piece, w[1], preferred_element_type=F32) * DH ** (-0.5)).astype(BF16)
        value = jnp.dot(piece, w[2], preferred_element_type=F32).astype(BF16)
        for h in range(heads):
            part = slice(h * head_width, (h + 1) * head_width)
            k, v = key[:, part], value[:, part]
            end = last[h : h + 1, :]
            grown = state[h]
            held[h] = grown.astype(BF16)
            faded = (k.astype(F32) * jnp.exp(end - by_row[:, h : h + 1])).astype(BF16)
            state[h] = jnp.exp(end) * grown + contract(faded, v, ((0,), (0,)))

        @pl.when(jnp.logical_and(place == 0, c == chunks - 1))
        def _():
            state_out[...] = state[...].astype(BF16)
            if n_seq > 1:
                s_copy.start()

        query = jnp.dot(piece, w[0], preferred_element_type=F32).astype(BF16)
        for h in range(heads):
            part = slice(h * head_width, (h + 1) * head_width)
            q, k, v = query[:, part], key[:, part], value[:, part]
            col = by_row[:, h : h + 1]
            mask = jnp.exp(jnp.where(causal, col - running[h : h + 1, :], -1e30))
            scores = (contract(q, k, ((1,), (1,))) * mask).astype(BF16)
            qf = q.astype(F32)
            carried = jnp.dot((qf * jnp.exp(col)).astype(BF16), held[h], preferred_element_type=F32)
            local_out[here, part] = jnp.dot(scores, v, preferred_element_type=F32) + carried
            q_in[here, part] = (qf * jnp.exp(col + before[h : h + 1, 0:1])).astype(BF16)
        offset[...] = before + last

    @pl.when(place == 0)
    def _():
        enter[...] = jnp.zeros_like(enter)

    def owner(o):
        t, s = o // 2, o % 2
        return lax.rem(chip + t + 1, chips) * 2 + lax.rem(core + s + (t + 1) // chips, 2)

    def gate_of(step):
        o, r = lax.rem(step, n_mp), step // n_mp
        here = at_rows(owner(o) * parts + r)
        g = jnp.dot(x[here, :], w[3], preferred_element_type=F32).astype(BF16).astype(F32)
        gates[...] = g / (1.0 + jnp.exp(-g))

    weights[3].wait()
    gate_of(0)

    @pl.when(place > 0)
    def _():
        s_copy.wait_recv()
        enter[...] = state_got[...]

    if n_seq > 2:
        @pl.when(jnp.logical_and(place > 0, place < n_seq - 1))
        def _():
            for h in range(heads):
                total = jnp.exp(offset[h : h + 1, 0:1])
                state_out[h] = (total * enter[h].astype(F32) + state[h]).astype(BF16)
            s_copy.start()

    def m_copy(o, r):
        to = owner(o)
        return pltpu.make_async_remote_copy(
            src_ref=moved.at[at_rows(to * parts + r), :], dst_ref=got.at[me, at_rows(r), :],
            send_sem=m_send.at[o, r], recv_sem=m_recv.at[me, r],
            device_id={"mp": to}, device_id_type=MESH)

    def q_copy(o, r):
        to = owner(o)
        return pltpu.make_async_remote_copy(
            src_ref=sq_out.at[to * parts + r], dst_ref=sq_got.at[me, r],
            send_sem=q_send.at[o, r], recv_sem=q_recv.at[me, r],
            device_id={"mp": to}, device_id_type=MESH)

    steps = n_mp * parts
    ones = jnp.ones((8, width), BF16)

    @pl.loop(0, steps)
    def _(step):
        o, r = lax.rem(step, n_mp), step // n_mp
        block = owner(o) * parts + r
        here = at_rows(block)
        kept = []
        for h in range(heads):
            part = slice(h * head_width, (h + 1) * head_width)
            whole = local_out[here, part] + jnp.dot(q_in[here, part], enter[h], preferred_element_type=F32)
            kept.append(whole.astype(BF16))
            moved[here, part] = (gates[:, part] * kept[h].astype(F32)).astype(BF16)

        @pl.when(o < n_mp - 1)
        def _():
            m_copy(o, r).start()

        squares = jnp.zeros((8, rows), F32)
        for h in range(heads):
            square = kept[h].astype(F32) * kept[h].astype(F32)
            high = square.astype(BF16)
            low = (square - high.astype(F32)).astype(BF16)
            unit = ones[:, h * head_width : (h + 1) * head_width]
            squares += contract(unit, high, ((1,), (1,))) + contract(unit, low, ((1,), (1,)))
        sq_out[block] = squares

        @pl.when(o < n_mp - 1)
        def _():
            q_copy(o, r).start()

        @pl.when(o == n_mp - 1)
        def _():
            got[me, at_rows(r), :] = moved[here, :]
            sq_got[me, r] = squares

        @pl.when(step < steps - 1)
        def _():
            gate_of(step + 1)

    def m_arrival(source, r):
        there = got.at[source, at_rows(r), :]
        return pltpu.make_async_remote_copy(
            src_ref=there, dst_ref=there, send_sem=m_send.at[0, r], recv_sem=m_recv.at[source, r],
            device_id={"mp": partner}, device_id_type=MESH)

    def q_arrival(source, r):
        there = sq_got.at[source, r]
        return pltpu.make_async_remote_copy(
            src_ref=there, dst_ref=there, send_sem=q_send.at[0, r], recv_sem=q_recv.at[source, r],
            device_id={"mp": partner}, device_id_type=MESH)

    for r in range(parts):
        for other in range(1, n_mp):
            source = lax.rem(me + other, n_mp)
            q_arrival(source, r).wait_recv()
            m_arrival(source, r).wait_recv()
        total = sq_got[0, r]
        for source in range(1, n_mp):
            total += sq_got[source, r]
        scale = lax.rsqrt(total * (1.0 / (n_mp * width)) + 1e-06).T[:, 0:1]
        span = slice(r * rows, (r + 1) * rows)
        for source in range(n_mp):
            part = slice(source * width, (source + 1) * width)
            out[span, part] = (got[source, span, :].astype(F32) * scale * gain[:, part]).astype(BF16)

    @pl.loop(0, chunks)
    def _(c):
        for step in range(1, chips):
            y_copy(c, step).wait_send()
        for step in range(chips):
            d_copy(c, step).wait_send()

    @pl.loop(0, n_mp - 1)
    def _(o):
        for r in range(parts):
            q_copy(o, r).wait_send()
            m_copy(o, r).wait_send()

    if n_seq > 1:
        @pl.when(place < n_seq - 1)
        def _():
            s_copy.wait_send()


def body(n_mp, n_seq, tokens, w_query, w_key, w_value, w_gate, decay_exponent, forget, norm_gain):
    seq_rows, width = tokens.shape
    features = w_query.shape[0]
    heads = decay_exponent.shape[0]
    own_rows = seq_rows // n_mp
    rows = 256 if own_rows % 256 == 0 else own_rows
    chunks, parts = seq_rows // rows, own_rows // rows
    rate = jnp.log1p(-jnp.exp2(-decay_exponent.astype(F32)))
    hbm, vmem = pl.BlockSpec(memory_space=pl.ANY), pl.BlockSpec(memory_space=pltpu.VMEM)
    dma = pltpu.SemaphoreType.DMA
    chips = n_mp // 2
    return pl.pallas_call(
        functools.partial(kernel, n_mp, n_seq, heads, rows),
        out_shape=jax.ShapeDtypeStruct((own_rows, features), BF16),
        in_specs=[hbm] * 5 + [vmem] * 3,
        out_specs=vmem,
        scratch_shapes=[
            pltpu.VMEM((seq_rows, features), BF16),
            pltpu.VMEM((4, features, width), BF16),
            pltpu.VMEM((seq_rows, width), F32),
            pltpu.VMEM((seq_rows, width), BF16),
            pltpu.VMEM((seq_rows, width), BF16),
            pltpu.VMEM((n_mp, own_rows, width), BF16),
            pltpu.VMEM((chunks, 8, rows), F32),
            pltpu.VMEM((n_mp, parts, 8, rows), F32),
            pltpu.VMEM((rows, width), F32),
            pltpu.VMEM((heads, DH, DH), F32),
            pltpu.VMEM((heads, DH, DH), BF16),
            pltpu.VMEM((heads, DH, DH), BF16),
            pltpu.VMEM((heads, DH, DH), BF16),
            pltpu.VMEM((heads, DH, DH), BF16),
            pltpu.VMEM((heads, 128), F32),
            dma((4,)),
            dma((chunks,)),
            dma((chunks, chips)),
            dma((chunks, chips)),
            dma((chunks, chips)),
            dma((chunks, chips)),
            dma,
            dma,
            dma((n_mp, parts)),
            dma((n_mp, parts)),
            dma((n_mp, parts)),
            dma((n_mp, parts)),
        ],
        compiler_params=pltpu.CompilerParams(
            collective_id=0, has_side_effects=True, vmem_limit_bytes=60 * 1024 * 1024
        ),
    )(tokens, w_query, w_key, w_value, w_gate, forget.T, rate[:, None], norm_gain[None, :])


def solution(mesh):
    placed = (
        P(("dp", "seq"), "mp"),
        P(None, "mp"),
        P(None, "mp"),
        P(None, "mp"),
        P(None, "mp"),
        P("mp"),
        P(("dp", "seq"), "mp"),
        P(),
    )
    return jax.shard_map(
        functools.partial(body, mesh.shape["mp"], mesh.shape["seq"]),
        mesh=mesh,
        in_specs=placed,
        out_specs=P(("dp", "seq", "mp"), None),
        check_vma=False,
    )
```
